128 devices in a mesh: grp: 4 (over z), seq: 32 (over x, y, core).
Axes of the slice: x: 4, y: 4, z: 4, core: 2. Of those that a mesh axis runs over, the one named last changes fastest.
Arguments:
- hidden_in: bfloat16 [96, 4096], P(None, ('grp', 'seq')), may hold values from -6 to 6
- norm_gain: float32 [4096], replicated, may hold values from 0.5 to 1.5
- w_ssm_in: bfloat16 [4096, 8192], P(None, ('grp', 'seq')), may hold values from -0.09375 to 0.09375
- w_ssm_gate: bfloat16 [4096, 8192], P(None, ('grp', 'seq')), may hold values from -0.09375 to 0.09375
- conv_weight: float32 [4, 8192], P(None, ('grp', 'seq')), may hold values from -3 to 3
- conv_bias: float32 [8192], P(('grp', 'seq')), may hold values from -0.5 to 0.5
- conv_state: bfloat16 [96, 3, 8192], P(None, None, ('grp', 'seq')), may hold values from -6 to 6
- w_state_proj: bfloat16 [8192, 288], P(('grp', 'seq')), may hold values from -0.0625 to 0.0625
- w_step: bfloat16 [256, 8192], P(None, ('grp', 'seq')), may hold values from -0.375 to 0.375
- step_bias: float32 [8192], P(('grp', 'seq')), may hold values from -4 to -1
- log_decay: float32 [16, 8192], P(None, ('grp', 'seq')), may hold values from 0 to 2.7
- skip_gain: float32 [8192], P(('grp', 'seq')), may hold values from 0.5 to 1.5
- ssm_state: float32 [96, 16, 8192], P(None, None, ('grp', 'seq')), may hold values from -6 to 6
- w_ssm_out: bfloat16 [8192, 4096], P(('grp', 'seq')), may hold values from -0.25 to 0.25
- w_query: bfloat16 [4096, 2048], P(None, 'grp'), may hold values from -6 to 6
- key_projection: bfloat16 [4096, 1024], P(None, 'grp'), may hold values from -0.09375 to 0.09375
- value_projection: bfloat16 [4096, 1024], P(None, 'grp'), may hold values from -0.09375 to 0.09375
- w_attn_out: bfloat16 [2048, 4096], P('grp', 'seq'), may hold values from -0.125 to 0.125
- w_mlp_gate: bfloat16 [4096, 14336], P(None, ('grp', 'seq')), may hold values from -0.09375 to 0.09375
- w_mlp_up: bfloat16 [4096, 14336], P(None, ('grp', 'seq')), may hold values from -0.09375 to 0.09375
- w_mlp_down: bfloat16 [14336, 4096], P(('grp', 'seq')), may hold values from -0.1875 to 0.1875
- cached_inputs: bfloat16 [96, 512, 4096], P('seq'), may hold values from -6 to 6
- window_lengths: int32 [96], replicated, may hold values from 1 to 512, as said below
Outputs:
- hidden_out: bfloat16 [96, 4096], P(None, ('grp', 'seq'))
- state_out: float32 [96, 16, 8192], P(None, None, ('grp', 'seq'))
The draws below stay inside these ranges and needn't reach their ends.
Inputs may be any that keep to these rules, and one draw needn't show every extreme that they name: `window_lengths`: every sequence has at least one valid cached position, and some sequence fills the whole window of 512.
All inputs are finite; a program needn't handle non-finite values.
Results may differ from the reference program's by a relative error of at most 0.012.
The reference program's roundings to bfloat16 on the way count: a program that leaves them out, or rounds other values in their place, can miss the bound.
Values may be sent and summed in bfloat16 or wider, within the bound.
A program may use at most 128 MiB of HBM per device.

```python
import jax
import jax.numpy as jnp
from jax import lax

MODEL_DIM = 4096
E = 8192
NS = 16
KC = 4
DTR = 256
QUERY_HEADS = 16
KEY_VALUE_HEADS = 8
HEAD_SIZE = 128
FF = 14336
WINDOW_SPAN = 512
BATCH_SEQUENCES = 96


def draw_window_lengths(key, part):
    drawn_lengths = jax.random.randint(jax.random.fold_in(key, 7), (BATCH_SEQUENCES,), 1, WINDOW_SPAN + 1, dtype=jnp.int32)
    chosen = jax.random.randint(jax.random.fold_in(key, 11), (), 0, BATCH_SEQUENCES, dtype=jnp.int32)
    return jnp.where(jnp.arange(BATCH_SEQUENCES, dtype=jnp.int32) == chosen, WINDOW_SPAN, drawn_lengths).astype(jnp.int32)


def draw_w_query(key, part):
    columns = QUERY_HEADS * HEAD_SIZE
    chosen_heads = jax.random.permutation(jax.random.fold_in(key, 3), QUERY_HEADS)
    entries = jax.random.normal(jax.random.fold_in(key, 5), (MODEL_DIM, columns), jnp.float32)
    levels = jnp.array([24.0, 48.0, 96.0], jnp.float32)
    head_scale = jnp.ones((QUERY_HEADS,), jnp.float32).at[chosen_heads[:3]].set(levels)
    column_scale = jnp.repeat(head_scale, HEAD_SIZE)
    scaled = entries * column_scale[None, :] * float(MODEL_DIM) ** (-0.5)
    return jnp.clip(scaled, -6.0, 6.0).astype(jnp.bfloat16)


def spiked(values, key, source, target, blocks, factor):
    def block_of(axis_at):
        return (jnp.arange(values.shape[axis_at]) // (values.shape[axis_at] // blocks)).reshape((-1,) + (1,) * (values.ndim - 1 - axis_at))

    one_side = jax.random.permutation(key, blocks)[block_of(target)]
    far = (block_of(target) + blocks // 2) % blocks
    return jnp.where((block_of(source) == one_side) | (block_of(source) == far), factor * values, values)


def level_of(stream_key, dims, shards, least, high):
    loudness, own = 1.0, jax.random.fold_in(stream_key, 6)
    for dim, shards_of in shards:
        draws = jnp.exp(jax.random.uniform(jax.random.fold_in(own, dim), (shards_of,), jnp.float32, least / len(shards), high / len(shards)))
        loudness = loudness * jnp.repeat(draws, dims[dim] // shards_of).reshape([-1 if axis == dim else 1 for axis in range(len(dims))])
    return loudness


def bell_draw(stream_key, dims, scale, reach, pieces=(), held_as=jnp.bfloat16):
    level = level_of(stream_key, dims, pieces, -0.22, 0.18) if pieces else 1.0
    values = jax.random.normal(stream_key, dims, jnp.float32) * scale * level
    return jnp.minimum(jnp.maximum(values, -reach), reach).astype(held_as)


def noise_with(rng, extent, deviation, limit, shards, heavy, kind=jnp.bfloat16):
    drawn = deviation * jax.random.normal(rng, extent, jnp.float32)
    if shards:
        drawn = drawn * level_of(rng, extent, shards, -0.22, 0.18)
    return jnp.clip(spiked(drawn, jax.random.fold_in(rng, 3), *heavy), -limit, limit).astype(kind)


def setup_inputs(seed: int = 0) -> dict:
    key_list = jax.random.split(jax.random.key(seed), 24)
    return {
        "hidden_in": bell_draw(key_list[0], (BATCH_SEQUENCES, MODEL_DIM), 1.0, 6.0, ((1, 128),)),
        "norm_gain": jnp.clip(1.0 + 0.1 * jax.random.normal(key_list[1], (MODEL_DIM,), jnp.float32), 0.5, 1.5),
        "w_ssm_in": bell_draw(key_list[2], (MODEL_DIM, E), MODEL_DIM ** -0.5, 0.09375, ((1, 128),)),
        "w_ssm_gate": bell_draw(key_list[3], (MODEL_DIM, E), MODEL_DIM ** -0.5, 0.09375, ((1, 128),)),
        "conv_weight": bell_draw(key_list[4], (KC, E), KC ** -0.5, 3.0, ((1, 128),), jnp.float32),
        "conv_bias": jnp.clip(jax.random.uniform(key_list[5], (E,), jnp.float32, -0.5, 0.5) * level_of(key_list[5], (E,), ((0, 128),), -0.4, 0.0), -0.5, 0.5),
        "conv_state": bell_draw(key_list[6], (BATCH_SEQUENCES, KC - 1, E), 1.0, 6.0, ((2, 128),)),
        "w_state_proj": bell_draw(key_list[7], (E, DTR + 2 * NS), E ** -0.5, 0.0625, ((0, 128),)),
        "w_step": bell_draw(key_list[8], (DTR, E), DTR ** -0.5, 0.375, ((1, 128),)),
        "step_bias": jnp.clip(-4.0 + 3.0 * jax.random.uniform(key_list[9], (E,), jnp.float32) ** level_of(key_list[9], (E,), ((0, 128),), -0.2, 0.2), -4.0, -1.0),
        "log_decay": jnp.clip(2.7 * jax.random.uniform(key_list[10], (NS, E), jnp.float32) ** level_of(key_list[10], (NS, E), ((1, 128),), -0.2, 0.2), 0.0, 2.7),
        "skip_gain": jnp.clip(0.5 + 1.0 * jax.random.uniform(key_list[11], (E,), jnp.float32) ** level_of(key_list[11], (E,), ((0, 128),), -0.2, 0.2), 0.5, 1.5),
        "ssm_state": bell_draw(key_list[12], (BATCH_SEQUENCES, NS, E), 1.0, 6.0, ((2, 128),), jnp.float32),
        "w_ssm_out": noise_with(key_list[13], (E, MODEL_DIM), E ** -0.5, 0.25, ((0, 128),), (0, 1, 128, 5.5)),
        "w_query": draw_w_query(jax.random.fold_in(key_list[23], 71), 0),
        "key_projection": bell_draw(key_list[15], (MODEL_DIM, KEY_VALUE_HEADS * HEAD_SIZE), MODEL_DIM ** -0.5, 0.09375, ((1, 4),)),
        "value_projection": bell_draw(key_list[16], (MODEL_DIM, KEY_VALUE_HEADS * HEAD_SIZE), MODEL_DIM ** -0.5, 0.09375, ((1, 4),)),
        "w_attn_out": bell_draw(key_list[17], (QUERY_HEADS * HEAD_SIZE, MODEL_DIM), (QUERY_HEADS * HEAD_SIZE) ** -0.5, 0.125, ((0, 4), (1, 32))),
        "w_mlp_gate": bell_draw(key_list[18], (MODEL_DIM, FF), MODEL_DIM ** -0.5, 0.09375, ((1, 128),)),
        "w_mlp_up": bell_draw(key_list[19], (MODEL_DIM, FF), MODEL_DIM ** -0.5, 0.09375, ((1, 128),)),
        "w_mlp_down": noise_with(key_list[20], (FF, MODEL_DIM), FF ** -0.5, 0.1875, ((0, 128),), (0, 1, 128, 5.5)),
        "cached_inputs": bell_draw(key_list[21], (BATCH_SEQUENCES, WINDOW_SPAN, MODEL_DIM), 1.0, 6.0, ((0, 32),)),
        "window_lengths": draw_window_lengths(jax.random.fold_in(key_list[23], 71), 0),
    }


epsilon = 1e-05
rope_base = 10000.0

def apply_rotary(head_values, positions):
    half_dim = head_values.shape[-1] // 2
    frequency = rope_base ** (-(jnp.arange(half_dim, dtype=jnp.float32) * 2.0) / head_values.shape[-1])
    angles = positions[..., None, None] * frequency
    cosine = jnp.cos(angles)
    sine_part = jnp.sin(angles)
    front_half = head_values[..., :half_dim]
    back_half = head_values[..., half_dim:]
    return jnp.concatenate([front_half * cosine - back_half * sine_part, back_half * cosine + front_half * sine_part], axis=-1)

def reference(hidden_in, norm_gain, w_ssm_in, w_ssm_gate, conv_weight, conv_bias, conv_state, w_state_proj, w_step, step_bias, log_decay, skip_gain, ssm_state, w_ssm_out, w_query, key_projection, value_projection, w_attn_out, w_mlp_gate, w_mlp_up, w_mlp_down, cached_inputs, window_lengths):
    hidden_f = hidden_in.astype(jnp.float32)
    row_scale = lax.rsqrt(lax.optimization_barrier(jnp.mean(hidden_f * hidden_f, axis=1, keepdims=True)) + epsilon)
    normed_input = (hidden_f * row_scale * norm_gain).astype(jnp.bfloat16)
    ssm_input = jnp.dot(normed_input, w_ssm_in, preferred_element_type=jnp.float32).astype(jnp.bfloat16)
    gate_input = jnp.dot(normed_input, w_ssm_gate, preferred_element_type=jnp.float32)
    past_inputs = conv_state.astype(jnp.float32)
    conv_sum = conv_bias + lax.optimization_barrier(jnp.sum(past_inputs * conv_weight[:-1][None], axis=1)) + conv_weight[-1] * lax.optimization_barrier(ssm_input).astype(jnp.float32)
    conv_out = jax.nn.silu(conv_sum)
    low_rank = jnp.dot(conv_out.astype(jnp.bfloat16), w_state_proj, preferred_element_type=jnp.float32)
    step_low = low_rank[:, :DTR].astype(jnp.bfloat16)
    input_map = low_rank[:, DTR:DTR + NS]
    output_map = low_rank[:, DTR + NS:]
    step_size = jax.nn.softplus(jnp.dot(step_low, w_step, preferred_element_type=jnp.float32) + step_bias)
    decay_rate = jnp.exp(log_decay)
    state_out = jnp.exp(-step_size[:, None, :] * decay_rate[None]) * ssm_state + step_size[:, None, :] * input_map[:, :, None] * conv_out[:, None, :]
    ssm_mixed = lax.optimization_barrier(jnp.sum(state_out * output_map[:, :, None], axis=1)) + skip_gain * conv_out
    ssm_gated = (ssm_mixed * jax.nn.silu(gate_input)).astype(jnp.bfloat16)
    ssm_term = jnp.dot(ssm_gated, w_ssm_out, preferred_element_type=jnp.float32)
    gate_act = jnp.dot(normed_input, w_mlp_gate, preferred_element_type=jnp.float32)
    up_act = jnp.dot(normed_input, w_mlp_up, preferred_element_type=jnp.float32)
    mlp_hidden = (jax.nn.silu(gate_act) * up_act).astype(jnp.bfloat16)
    mlp_term = jnp.dot(mlp_hidden, w_mlp_down, preferred_element_type=jnp.float32)
    fresh_position = window_lengths.astype(jnp.float32)
    query = apply_rotary(jnp.dot(normed_input, w_query, preferred_element_type=jnp.float32).reshape(BATCH_SEQUENCES, QUERY_HEADS, HEAD_SIZE), fresh_position).astype(jnp.bfloat16)
    fresh_key = apply_rotary(jnp.dot(normed_input, key_projection, preferred_element_type=jnp.float32).reshape(BATCH_SEQUENCES, KEY_VALUE_HEADS, HEAD_SIZE), fresh_position).astype(jnp.bfloat16)
    fresh_value = jnp.dot(normed_input, value_projection, preferred_element_type=jnp.float32).astype(jnp.bfloat16).reshape(BATCH_SEQUENCES, KEY_VALUE_HEADS, HEAD_SIZE)
    heads_per_group = QUERY_HEADS // KEY_VALUE_HEADS
    attention_scale = HEAD_SIZE ** (-0.5)

    def one_row(row_args):
        window_row_inputs, query_for_row, row_key, row_value, row_length = row_args
        slot_ids = jnp.arange(WINDOW_SPAN, dtype=jnp.int32)
        window_key_rows = jnp.dot(window_row_inputs, key_projection, preferred_element_type=jnp.float32).reshape(WINDOW_SPAN, KEY_VALUE_HEADS, HEAD_SIZE)
        window_key_rows = apply_rotary(window_key_rows, slot_ids.astype(jnp.float32)).astype(jnp.bfloat16)
        window_value_rows = jnp.dot(window_row_inputs, value_projection, preferred_element_type=jnp.float32).astype(jnp.bfloat16).reshape(WINDOW_SPAN, KEY_VALUE_HEADS, HEAD_SIZE)
        grouped_query = query_for_row.astype(jnp.float32).reshape(KEY_VALUE_HEADS, heads_per_group, HEAD_SIZE)
        scores = jnp.einsum('kgd,wkd->kgw', grouped_query, window_key_rows.astype(jnp.float32)) * attention_scale
        fresh_score = jnp.einsum('kgd,kd->kg', grouped_query, row_key.astype(jnp.float32)) * attention_scale
        is_valid = slot_ids < row_length
        scores = jnp.where(is_valid[None, None, :], scores, -1e+30)
        row_max = jnp.maximum(lax.optimization_barrier(jnp.max(scores, axis=-1)), fresh_score)
        weights = jnp.where(is_valid[None, None, :], jnp.exp(scores - row_max[..., None]), 0.0)
        weight_new = jnp.exp(fresh_score - row_max)
        row_total = lax.optimization_barrier(jnp.sum(weights, axis=-1)) + weight_new
        weighted = jnp.einsum('kgw,wkd->kgd', weights, window_value_rows.astype(jnp.float32)) + weight_new[..., None] * row_value.astype(jnp.float32)[:, None, :]
        return (weighted / row_total[..., None]).reshape(QUERY_HEADS * HEAD_SIZE).astype(jnp.bfloat16)
    attended = lax.map(one_row, (cached_inputs, query, fresh_key, fresh_value, window_lengths))
    attn_term = jnp.dot(attended, w_attn_out, preferred_element_type=jnp.float32)
    hidden_out = (hidden_f + (ssm_term + mlp_term + attn_term)).astype(jnp.bfloat16)
    return (hidden_out, state_out)
```

```python
import functools

import jax
import jax.numpy as jnp
import numpy as np
from jax import lax
from jax.experimental import pallas as pl
from jax.experimental.pallas import tpu as pltpu
from jax.sharding import Mesh
from jax.sharding import PartitionSpec as P

HEAD = 128
EPS = 1e-05
ROPE_BASE = 10000.0
MESH_ID = pl.DeviceIdType.MESH
F32, BF16 = jnp.float32, jnp.bfloat16
GRP_SEQ = ("grp", "seq_0", "seq_1", "seq_2")
SEQ = ("seq_0", "seq_1", "seq_2")
DOT_00 = (((0,), (0,)), ((), ()))
DOT_11 = (((1,), (1,)), ((), ()))
NAMES = (
    "hid", "gain", "w_in", "w_gate", "conv_w", "conv_b", "conv_st", "w_sp", "w_step", "step_b",
    "log_decay", "skip", "state", "w_so", "w_q", "w_k", "w_v", "w_ao", "w_mg", "w_mu", "w_md",
    "cached", "lens", "cos", "sin", "pick",
)


def silu(v):
    return v * jax.nn.sigmoid(v)


def rot(v, cosine, sine):
    return v * cosine + pltpu.roll(v, HEAD // 2, 1) * sine


def dot(a, b):
    return jnp.dot(a, b, preferred_element_type=F32)


def dot_g(a, b, dims):
    return lax.dot_general(a, b, dims, preferred_element_type=F32)


def kernel(sizes, *refs):
    nz, nx, ny, batch, own_seqs, window = sizes
    n_in = len(NAMES)
    r = dict(zip(NAMES, refs[:n_in]))
    out_ref, state_out = refs[n_in : n_in + 2]
    (
        X, XN, G, xb, wkv, wq, wst, wsp, wstep, wso, wmd, wao, kbuf, vbuf, cos, sin, pick,
        gain, conv_w, conv_b, conv_st, step_b, log_decay, skip, state, att_f, AT, LD, LR, LS, RL,
        LF, Pf, PB, R0, A1, B0, B1, A20, A21, C0, C1, A30, A31, D0, D1, gated, mlph,
        lsem, ags, agr, agds, agdr, ars, arr, ards, ardr, ats, atr, rss, rsr, rsds, rsdr,
    ) = refs[n_in + 2 :]
    nzx = nz * nx
    z, x = lax.axis_index("grp"), lax.axis_index("seq_0")
    y, c = lax.axis_index("seq_1"), lax.axis_index("seq_2")
    pc = 1 - c
    zx = z * nx + x
    seq = (x * ny + y) * 2 + c
    at = {"grp": z, "seq_0": x, "seq_1": y}
    count = {"grp": nz, "seq_0": nx, "seq_1": ny}
    ch = wst.shape[0]
    e_dim = wso.shape[0]
    ff = wmd.shape[0]
    sends = []

    def send(src, dst, ss, rs, axis, d):
        to = pc if axis == "seq_2" else lax.rem(at[axis] + d, count[axis])
        copy = pltpu.make_async_remote_copy(
            src_ref=src, dst_ref=dst, send_sem=ss, recv_sem=rs,
            device_id={axis: to}, device_id_type=MESH_ID,
        )
        copy.start()
        sends.append(copy)
        return copy

    def source(axis, d):
        return lax.rem(at[axis] + count[axis] - d, count[axis])

    local = {}

    def fetch(key, src, dst):
        copy = pltpu.make_async_copy(src, dst, lsem.at[len(local)])
        copy.start()
        local[key] = copy

    def ready(*keys):
        for key in keys:
            local[key].wait()

    for h in range(2):
        fetch(("hid", h), r["hid"].at[pl.ds(16 * h, 16)], X.at[h, c, zx, y])
    kvw = r["w_k"].shape[1]
    fetch("wk", r["w_k"], wkv.at[:, pl.ds(0, kvw)])
    fetch("wv", r["w_v"], wkv.at[:, pl.ds(kvw, kvw)])
    chunk = min(256, window)
    n_chunks = own_seqs * window // chunk
    for i in range(n_chunks):
        rows = pl.ds(i * chunk, chunk)
        fetch(("xb", i), r["cached"].at[rows], xb.at[rows])
        if i == 0:
            fetch("cos", r["cos"], cos)
            fetch("sin", r["sin"], sin)
    fetch("gain", r["gain"], gain)
    fetch("w_in", r["w_in"], wst.at[pl.ds(0, e_dim)])
    fetch("w_gate", r["w_gate"], wst.at[pl.ds(e_dim, e_dim)])
    for key, dst in (
        ("conv_w", conv_w), ("conv_b", conv_b), ("conv_st", conv_st), ("w_sp", wsp),
        ("step_b", step_b), ("log_decay", log_decay), ("skip", skip), ("w_q", wq),
    ):
        fetch(key, r[key], dst)
    fetch("w_mg", r["w_mg"], wst.at[pl.ds(2 * e_dim, ff)])
    fetch("w_mu", r["w_mu"], wst.at[pl.ds(2 * e_dim + ff, ff)])
    for key, dst in (
        ("w_md", wmd), ("w_step", wstep), ("state", state), ("w_so", wso), ("w_ao", wao), ("pick", pick),
    ):
        fetch(key, r[key], dst)

    barrier = pltpu.get_barrier_semaphore()
    for axis in ("grp", "seq_0", "seq_1"):
        for d in range(1, count[axis]):
            to = lax.rem(at[axis] + d, count[axis])
            pl.semaphore_signal(barrier, inc=1, device_id={axis: to}, device_id_type=MESH_ID)
    pl.semaphore_signal(barrier, inc=1, device_id={"seq_2": pc}, device_id_type=MESH_ID)
    pl.semaphore_wait(barrier, nz + nx + ny - 2)

    orders = (("seq_1", "seq_0", "grp"), ("seq_0", "grp", "seq_1"))

    def gathered(h, phase, zz, xx, yy):
        if phase == 0:
            return X.at[h, c, zz * nx + xx, yy]
        if h == 0:
            return X.at[0, c, zz * nx + xx] if phase == 1 else X.at[0, c, pl.ds(zz * nx, nx)]
        return X.at[1, c, pl.ds(zz * nx, nx), yy] if phase == 1 else X.at[1, c, :, yy]

    def gather_start(h, phase):
        ref = gathered(h, phase, z, x, y)
        axis = orders[h][phase]
        return [
            send(ref, ref, ags.at[h, phase, d - 1], agr.at[h, phase, d - 1], axis, d)
            for d in range(1, count[axis])
        ]

    ready(("hid", 0), ("hid", 1))
    gather = [gather_start(h, 0) for h in range(2)]

    def project(i, carry):
        rows = pl.ds(pl.multiple_of(i * chunk, chunk), chunk)
        kv = dot(xb[rows, :], wkv[...])
        place = pl.ds(pl.multiple_of(lax.rem(i, window // chunk) * chunk, chunk), chunk)
        cs, sn = cos[place, :], sin[place, :]
        for k in range(kvw // HEAD):
            cols = slice(k * HEAD, (k + 1) * HEAD)
            kbuf[rows, cols] = rot(kv[:, cols], cs, sn).astype(BF16)
        vbuf[rows, :] = kv[:, kvw:].astype(BF16)
        return carry

    def project_chunks(lo, hi):
        for i in range(lo, hi):
            ready(("xb", i))
        lax.fori_loop(lo, hi, project, 0)

    stop = (n_chunks // 3, n_chunks * 5 // 6)
    ready("wk", "wv", "cos", "sin")
    project_chunks(0, stop[0])
    for h in range(2):
        for copy in gather[h]:
            copy.wait_recv()
    gather = [gather_start(h, 1) for h in range(2)]
    project_chunks(stop[0], stop[1])
    for h in range(2):
        for copy in gather[h]:
            copy.wait_recv()
    gather = [gather_start(h, 2) for h in range(2)]
    across = []

    def cross(h, place, k):
        zz, yy = (place, y) if h == 0 else (z, place)
        ref = gathered(h, 2, zz, x, yy)
        across.append(send(ref, ref, agds.at[h, k], agdr.at[h, k], "seq_2", 0))

    cross(0, z, 0)
    cross(1, y, 0)
    project_chunks(stop[1], n_chunks)

    ready("gain", "conv_w", "conv_b", "conv_st", "w_sp", "step_b", "log_decay", "skip")
    for k in range(G.shape[0] // 128):
        G[k * 128 : (k + 1) * 128, :] = jnp.broadcast_to(gain[k : k + 1, :], (batch, 128)).T
    conv_wt = conv_w[...].T
    bias_col = conv_b[...].T
    step_col = step_b[...].T
    skip_col = skip[...].T
    decay = jnp.exp(log_decay[...]).T
    past = conv_wt[:, 0:1] * conv_st[0].astype(F32)
    for k in range(1, conv_st.shape[0]):
        past = past + conv_wt[:, k : k + 1] * conv_st[k].astype(F32)

    for k in (1, 3, 2):
        for h in range(2):
            axis = orders[h][2]
            if k < count[axis]:
                gather[h][k - 1].wait_recv()
                cross(h, source(axis, k), k)
    for copy in across:
        copy.wait_recv()

    def squares(i, acc):
        for h in range(2):
            for cc in range(2):
                for yy in range(ny):
                    v = X[h, cc, i, yy].astype(F32)
                    acc = acc + v * v
        return acc

    total = lax.fori_loop(0, nzx, squares, jnp.zeros((16, batch), F32))
    width = nzx * ny * 64
    scale = lax.rsqrt(jnp.sum(total, axis=0, keepdims=True) / width + EPS)

    def normalize(i, carry):
        for yy in range(ny):
            for cc in range(2):
                for h in range(2):
                    at_row = pl.multiple_of(i * (ny * 64), ny * 64) + (yy * 64 + cc * 32 + h * 16)
                    rows = pl.ds(pl.multiple_of(at_row, 16), 16)
                    v = X[h, cc, i, yy].astype(F32)
                    XN[rows, :] = (v * scale * G[rows, :]).astype(BF16)
        return carry

    lax.fori_loop(0, nzx, normalize, 0)

    ready("w_in", "w_gate")
    both = dot(wst[: 2 * e_dim, :], XN[...])
    ssm_in = both[:e_dim, :].astype(BF16).astype(F32)
    gate_in = both[e_dim:, :]
    conv_out = silu(bias_col + past + conv_wt[:, -1:] * ssm_in)
    low = dot_g(wsp[...], conv_out.astype(BF16), DOT_00)
    third = low.shape[0] // 6
    for cc in range(2):
        for t in range(3):
            LD[cc, t] = low[(cc * 3 + t) * third : (cc * 3 + t + 1) * third, :]
    low_first = send(LD.at[pc], LR, ards.at[0], ardr.at[0], "seq_2", 0)

    row = lax.broadcasted_iota(jnp.int32, (8, batch), 0)
    col = lax.broadcasted_iota(jnp.int32, (8, batch), 1)
    chosen = ((col == row + seq * own_seqs) & (row < own_seqs)).astype(F32).astype(BF16)
    fresh = dot_g(chosen, XN[...], DOT_11).astype(BF16)
    ready("w_q")
    query = dot(fresh, wq[...])
    new_kv = dot(fresh, wkv[...])

    low_first.wait_recv()
    for t in range(3):
        LS[0, t] = LD[c, t] + LR[t]
    ring = ("seq_0", "seq_1", "grp")

    def sum_start(phase):
        return [
            [
                send(LS.at[phase, t], RL.at[phase, t, d - 1], ars.at[phase, t, d - 1],
                     arr.at[phase, t, d - 1], ring[(t + phase) % 3], d)
                for d in range(1, count[ring[(t + phase) % 3]])
            ]
            for t in range(3)
        ]

    def sum_end(phase, copies):
        for t in range(3):
            value = LS[phase, t]
            for d, copy in enumerate(copies[t]):
                copy.wait_recv()
                value = value + RL[phase, t, d]
            if phase < 2:
                LS[phase + 1, t] = value
            else:
                LF[c, t] = value

    low_copies = sum_start(0)

    heads = query.shape[1] // HEAD
    kvs = kvw // HEAD
    per = heads // kvs
    row8 = lax.broadcasted_iota(jnp.int32, (8, HEAD), 0)
    slots = lax.broadcasted_iota(jnp.int32, (8, window), 1)
    cs = jnp.zeros((8, HEAD), F32)
    sn = jnp.zeros((8, HEAD), F32)
    lengths = []
    for b in range(own_seqs):
        length = r["lens"][seq * own_seqs + b]
        lengths.append(length)
        cs = jnp.where(row8 == b, cos[pl.ds(length, 1), :], cs)
        sn = jnp.where(row8 == b, sin[pl.ds(length, 1), :], sn)
    q_rot = [rot(query[:, h * HEAD : (h + 1) * HEAD], cs, sn).astype(BF16).astype(F32) for h in range(heads)]
    k_new = [rot(new_kv[:, k * HEAD : (k + 1) * HEAD], cs, sn).astype(BF16).astype(F32) for k in range(kvs)]
    v_new = [new_kv[:, kvw + k * HEAD : kvw + (k + 1) * HEAD].astype(BF16).astype(F32) for k in range(kvs)]
    unit = HEAD ** (-0.5)
    att_f[...] = jnp.zeros_like(att_f)
    for b in range(own_seqs):
        per_head = jnp.zeros((8, HEAD), F32)
        k_row = jnp.zeros((8, HEAD), F32)
        v_row = jnp.zeros((8, HEAD), F32)
        for h in range(heads):
            per_head = jnp.where(row8 == h, q_rot[h][b : b + 1, :], per_head)
            k_row = jnp.where(row8 == h, k_new[h // per][b : b + 1, :], k_row)
            v_row = jnp.where(row8 == h, v_new[h // per][b : b + 1, :], v_row)
        blocks = [jnp.where((row8 >= k * per) & (row8 < (k + 1) * per), per_head, 0.0) for k in range(kvs)]
        rows = slice(b * window, (b + 1) * window)
        scores = dot_g(jnp.concatenate(blocks, axis=1).astype(BF16), kbuf[rows, :], DOT_11) * unit
        fresh_score = jnp.sum(per_head * k_row, axis=1, keepdims=True) * unit
        valid = slots < lengths[b]
        scores = jnp.where(valid, scores, -1e30)
        top = jnp.maximum(jnp.max(scores, axis=1, keepdims=True), fresh_score)
        weights = jnp.where(valid, jnp.exp(scores - top), 0.0)
        weight_new = jnp.exp(fresh_score - top)
        all_weights = jnp.sum(weights, axis=1, keepdims=True) + weight_new
        mixed = dot(weights.astype(BF16), vbuf[rows, :])
        taken = mixed[:, :HEAD]
        for k in range(1, kvs):
            taken = jnp.where(row8 >= k * per, mixed[:, k * HEAD : (k + 1) * HEAD], taken)
        result = (taken + weight_new * v_row) / all_weights
        att_f[b * heads : (b + 1) * heads, :] = result[:heads, :]
    AT[c, x, y] = att_f[...].astype(BF16)

    def att_start(k):
        ref, axis = (AT.at[c, x, y], "seq_0") if k == 0 else (AT.at[c, :, y], "seq_1")
        return [send(ref, ref, ats.at[k, d - 1], atr.at[k, d - 1], axis, d) for d in range(1, count[axis])]

    att_copies = att_start(0)
    sum_end(0, low_copies)
    low_copies = sum_start(1)

    ready("w_mg", "w_mu")
    inner = dot(wst[2 * e_dim :, :], XN[...])
    mlph[...] = (silu(inner[:ff, :]) * inner[ff:, :]).astype(BF16)
    for copy in att_copies:
        copy.wait_recv()
    att_copies = att_start(1)
    sum_end(1, low_copies)
    low_copies = sum_start(2)
    ready("w_md")
    span = ny * 64

    def down(i, carry):
        rows = pl.ds(pl.multiple_of(i * span, span), span)
        Pf[rows, :] = dot_g(wmd[:, rows], mlph[...], DOT_00)
        return carry

    lax.fori_loop(0, nzx, down, 0)
    for copy in att_copies:
        copy.wait_recv()
    att_last = send(AT.at[c], AT.at[c], ats.at[2, 0], atr.at[2, 0], "seq_2", 0)
    sum_end(2, low_copies)
    low_last = send(LF.at[c], LF.at[c], ards.at[1], ardr.at[1], "seq_2", 0)

    ready("w_ao", "pick")
    att_last.wait_recv()
    everyone = AT[...].reshape(-1, HEAD)
    part = jnp.zeros((batch, wao.shape[1]), F32)
    for h in range(heads):
        of_head = dot(pick[h * batch : (h + 1) * batch, :], everyone).astype(BF16)
        part = part + dot(of_head, wao[h * HEAD : (h + 1) * HEAD, :])
    n_cols = wao.shape[1]
    rows = pl.ds(pl.multiple_of(seq * n_cols, n_cols), n_cols)
    Pf[rows, :] = Pf[rows, :] + part.T

    ready("w_step", "state", "w_so")
    low_last.wait_recv()
    low = LF[...].reshape(6 * third, batch)
    rank = wstep.shape[1]
    n_state = state.shape[0]
    raw_step = dot(wstep[...], low[:rank, :].astype(BF16)) + step_col
    step = jnp.maximum(raw_step, 0.0) + jnp.log1p(jnp.exp(-jnp.abs(raw_step)))
    driven = step * conv_out
    mix = skip_col * conv_out
    for n in range(n_state):
        new = jnp.exp(-step * decay[:, n : n + 1]) * state[n] + driven * low[rank + n : rank + n + 1, :]
        state[n] = new
        mix = mix + new * low[rank + n_state + n : rank + n_state + n + 1, :]
    gated[...] = (mix * silu(gate_in)).astype(BF16)
    put_state = pltpu.make_async_copy(state, state_out, lsem.at[len(local)])
    put_state.start()

    def branch(i, carry):
        rows = pl.ds(pl.multiple_of(i * span, span), span)
        value = (dot_g(wso[:, rows], gated[...], DOT_00) + Pf[rows, :]).astype(BF16)
        for yy in range(ny):
            for cc in range(2):
                for h in range(2):
                    lo = yy * 64 + cc * 32 + h * 16
                    PB[cc, h, i, yy] = value[lo : lo + 16, :]
        return carry

    places = [lax.rem(z + 1 + k, nz) for k in range(nz)]
    cross_sum = []
    for k, zz in enumerate(places):
        lax.fori_loop(zz * nx, zz * nx + nx, branch, 0)
        planes = pl.ds(zz * nx, nx)
        cross_sum.append(
            send(PB.at[pc, :, planes], R0.at[:, planes], rsds.at[k], rsdr.at[k], "seq_2", 0)
        )

    def joined(i, carry):
        for h in range(2):
            A1[h, i] = (PB[c, h, i].astype(F32) + R0[h, i].astype(F32)).astype(BF16)
        return carry

    def reduce_send(h, phase, d, src, dst):
        axis = orders[h][2 - phase]
        return send(src, dst, rss.at[h, phase, d - 1], rsr.at[h, phase, d - 1], axis, d)

    first = [[], []]
    for k, zz in enumerate(places):
        cross_sum[k].wait_recv()
        lax.fori_loop(zz * nx, zz * nx + nx, joined, 0)
        if k < nz - 1:
            first[0].append(reduce_send(0, 0, k + 1, A1.at[0, pl.ds(zz * nx, nx)], B0.at[k]))
    for d in range(1, ny):
        first[1].append(reduce_send(1, 0, d, A1.at[1, :, lax.rem(y + d, ny)], B1.at[d - 1]))

    for copy in first[0]:
        copy.wait_recv()
    for xx in range(nx):
        value = A1[0, z * nx + xx].astype(F32)
        for d in range(nz - 1):
            value = value + B0[d, xx].astype(F32)
        A20[xx] = value.astype(BF16)
    second = [[], []]
    for d in range(1, nx):
        second[0].append(reduce_send(0, 1, d, A20.at[lax.rem(x + d, nx)], C0.at[d - 1]))
    for copy in first[1]:
        copy.wait_recv()
    for zz in range(nz):
        value = A1[1, zz * nx : (zz + 1) * nx, y].astype(F32)
        for d in range(ny - 1):
            value = value + B1[d, zz * nx : (zz + 1) * nx].astype(F32)
        A21[zz] = value.astype(BF16)
    for d in range(1, nz):
        second[1].append(reduce_send(1, 1, d, A21.at[lax.rem(z + d, nz)], C1.at[d - 1]))

    last = [[], []]
    for copy in second[0]:
        copy.wait_recv()
    value = A20[x].astype(F32)
    for d in range(nx - 1):
        value = value + C0[d].astype(F32)
    A30[...] = value.astype(BF16)
    for d in range(1, ny):
        last[0].append(reduce_send(0, 2, d, A30.at[lax.rem(y + d, ny)], D0.at[d - 1]))
    for copy in second[1]:
        copy.wait_recv()
    value = A21[z].astype(F32)
    for d in range(nz - 1):
        value = value + C1[d].astype(F32)
    A31[...] = value.astype(BF16)
    for d in range(1, nx):
        last[1].append(reduce_send(1, 2, d, A31.at[lax.rem(x + d, nx)], D1.at[d - 1]))

    for h, kept, place, landed in ((0, A30, y, D0), (1, A31, x, D1)):
        for copy in last[h]:
            copy.wait_recv()
        value = kept[place].astype(F32)
        for d in range(len(last[h])):
            value = value + landed[d].astype(F32)
        out_ref[h * 16 : (h + 1) * 16, :] = value
    for copy in sends:
        copy.wait_send()
    put_state.wait()


def tables(window):
    freq = np.float64(ROPE_BASE) ** (-(np.arange(HEAD // 2, dtype=np.float64) * 2.0) / HEAD)
    rows = -(-(window + 1) // 8) * 8
    angles = np.arange(rows, dtype=np.float64)[:, None] * freq.astype(np.float32).astype(np.float64)
    cosine, sine = np.cos(angles), np.sin(angles)
    cosine = np.concatenate([cosine, cosine], axis=1).astype(np.float32)
    sine = np.concatenate([-sine, sine], axis=1).astype(np.float32)
    return cosine, sine


def picker(nx, ny, own_seqs, heads):
    n_seq = nx * ny * 2
    out = np.zeros((heads, n_seq, own_seqs, 2, nx, ny, 16), np.float32)
    for s in range(n_seq):
        xx, yy, cc = s // (2 * ny), (s // 2) % ny, s % 2
        for b in range(own_seqs):
            for h in range(heads):
                out[h, s, b, cc, xx, yy, b * heads + h] = 1.0
    return out.reshape(heads * n_seq * own_seqs, n_seq * 16)


def per_device(shape, *args):
    nz, nx, ny = shape
    (
        hidden_in, norm_gain, w_ssm_in, w_ssm_gate, conv_weight, conv_bias, conv_state,
        w_state_proj, w_step, step_bias, log_decay, skip_gain, ssm_state, w_ssm_out, w_query,
        key_projection, value_projection, w_attn_out, w_mlp_gate, w_mlp_up, w_mlp_down,
        cached_inputs, window_lengths,
    ) = args
    batch = hidden_in.shape[0]
    width = norm_gain.shape[0]
    own_seqs, window = cached_inputs.shape[:2]
    e_dim, ff = w_ssm_in.shape[1], w_mlp_gate.shape[1]
    heads = w_query.shape[1] // HEAD
    kvw = key_projection.shape[1]
    taps, n_state = conv_weight.shape[0], log_decay.shape[0]
    nzx, n_low = nz * nx, w_state_proj.shape[1]
    third = n_low // 6
    cosine, sine = tables(window)
    picked = picker(nx, ny, own_seqs, heads)
    operands = (
        hidden_in.T, norm_gain.reshape(-1, 128), w_ssm_in.T, w_ssm_gate.T, conv_weight,
        conv_bias.reshape(1, -1), conv_state.transpose(1, 2, 0), w_state_proj, w_step.T,
        step_bias.reshape(1, -1), log_decay, skip_gain.reshape(1, -1), ssm_state.transpose(1, 2, 0),
        w_ssm_out, w_query, key_projection, value_projection, w_attn_out, w_mlp_gate.T, w_mlp_up.T,
        w_mlp_down, cached_inputs.reshape(own_seqs * window, width), window_lengths,
        jnp.asarray(cosine), jnp.asarray(sine), jnp.asarray(picked, BF16),
    )
    in_specs = [
        pl.BlockSpec(memory_space=pltpu.SMEM if name == "lens" else pl.ANY) for name in NAMES
    ]
    V, DMA = pltpu.VMEM, pltpu.SemaphoreType.DMA
    tail = (16, batch)
    scratch = [
        V((2, 2, nzx, ny) + tail, BF16),
        V((width, batch), BF16),
        V((width, batch), F32),
        V((own_seqs * window, width), BF16),
        V((width, 2 * kvw), BF16),
        V(w_query.shape, BF16),
        V((2 * e_dim + 2 * ff, width), BF16),
        V(w_state_proj.shape, BF16),
        V(w_step.shape[::-1], BF16),
        V(w_ssm_out.shape, BF16),
        V(w_mlp_down.shape, BF16),
        V(w_attn_out.shape, BF16),
        V((own_seqs * window, kvw), BF16),
        V((own_seqs * window, kvw), BF16),
        V(cosine.shape, F32),
        V(sine.shape, F32),
        V(picked.shape, BF16),
        V((width // 128, 128), F32),
        V((taps, e_dim), F32),
        V((1, e_dim), F32),
        V((taps - 1, e_dim, batch), BF16),
        V((1, e_dim), F32),
        V((n_state, e_dim), F32),
        V((1, e_dim), F32),
        V((n_state, e_dim, batch), F32),
        V((16, HEAD), F32),
        V((2, nx, ny, 16, HEAD), BF16),
        V((2, 3, third, batch), F32),
        V((3, third, batch), F32),
        V((3, 3, third, batch), F32),
        V((3, 3, 3, third, batch), F32),
        V((2, 3, third, batch), F32),
        V((width, batch), F32),
        V((2, 2, nzx, ny) + tail, BF16),
        V((2, nzx, ny) + tail, BF16),
        V((2, nzx, ny) + tail, BF16),
        V((nz - 1, nx, ny) + tail, BF16),
        V((ny - 1, nzx) + tail, BF16),
        V((nx, ny) + tail, BF16),
        V((nz, nx) + tail, BF16),
        V((nx - 1, ny) + tail, BF16),
        V((nz - 1, nx) + tail, BF16),
        V((ny,) + tail, BF16),
        V((nx,) + tail, BF16),
        V((ny - 1,) + tail, BF16),
        V((nx - 1,) + tail, BF16),
        V((e_dim, batch), BF16),
        V((ff, batch), BF16),
        DMA((48,)),
        DMA((2, 3, 3)), DMA((2, 3, 3)), DMA((2, 4)), DMA((2, 4)),
        DMA((3, 3, 3)), DMA((3, 3, 3)), DMA((2,)), DMA((2,)),
        DMA((3, 3)), DMA((3, 3)),
        DMA((2, 3, 3)), DMA((2, 3, 3)), DMA((4,)), DMA((4,)),
    ]
    summed, state = pl.pallas_call(
        functools.partial(kernel, (nz, nx, ny, batch, own_seqs, window)),
        out_shape=(
            jax.ShapeDtypeStruct((width // (nzx * ny * 2), batch), F32),
            jax.ShapeDtypeStruct((n_state, e_dim, batch), F32),
        ),
        in_specs=in_specs,
        out_specs=(pl.BlockSpec(memory_space=pltpu.VMEM), pl.BlockSpec(memory_space=pl.ANY)),
        scratch_shapes=scratch,
        compiler_params=pltpu.CompilerParams(
            collective_id=0, has_side_effects=True, vmem_limit_bytes=62 * 1024 * 1024
        ),
        name="block",
    )(*operands)
    hidden_out = (hidden_in.T.astype(F32) + summed).astype(BF16)
    return hidden_out.T, state.transpose(2, 0, 1)


def solution(mesh):
    nx = ny = 4
    if mesh.shape["seq"] != nx * ny * 2:
        nx = ny = 2
    nz = mesh.shape["grp"]
    torus = Mesh(mesh.devices.reshape(nz, nx, ny, 2), GRP_SEQ)
    placed = (
        P(None, GRP_SEQ),
        P(),
        P(None, GRP_SEQ),
        P(None, GRP_SEQ),
        P(None, GRP_SEQ),
        P(GRP_SEQ),
        P(None, None, GRP_SEQ),
        P(GRP_SEQ, None),
        P(None, GRP_SEQ),
        P(GRP_SEQ),
        P(None, GRP_SEQ),
        P(GRP_SEQ),
        P(None, None, GRP_SEQ),
        P(GRP_SEQ, None),
        P(None, "grp"),
        P(None, "grp"),
        P(None, "grp"),
        P("grp", SEQ),
        P(None, GRP_SEQ),
        P(None, GRP_SEQ),
        P(GRP_SEQ, None),
        P(SEQ, None, None),
        P(),
    )
    return jax.shard_map(
        functools.partial(per_device, (nz, nx, ny)),
        mesh=torus,
        in_specs=placed,
        out_specs=(P(None, GRP_SEQ), P(None, None, GRP_SEQ)),
        check_vma=False,
    )
```
